256 devices in a mesh: ctx: 8 (over z), vocab: 32 (over y, x, core).
Axes of the slice: x: 4, y: 4, z: 8, core: 2. Of those that a mesh axis runs over, the one named last changes fastest.
Arguments:
- hidden: bfloat16 [16, 128, 4096], P(None, 'ctx', 'vocab'), may hold values from -6 to 6
- head_weight: bfloat16 [4096, 128256], P(None, ('ctx', 'vocab')), may hold values from -0.09375 to 0.09375
- token_ids: int32 [16, 128], P(None, 'ctx'), may hold values from 0 to 128255
- response_mask: int32 [16, 128], P(None, 'ctx'), may hold values 0 or 1
- pair_order: int32 [16], replicated, may hold values from 0 to 15, each once
- frozen_logprob: float32 [16], replicated, may hold values from -40 to 40
Outputs:
- pair_loss: float32 [], replicated
- margins: float32 [8], replicated
- head_grad: bfloat16 [4096, 128256], P(None, ('ctx', 'vocab'))
- spread_grad: bfloat16 [4096, 128256], P(None, ('ctx', 'vocab'))
The draws below stay inside these ranges and needn't reach their ends.
Inputs may be any that keep to these rules, and one draw needn't show every extreme that they name: `token_ids`: token ids lie in 0 to 128255. `response_mask`: mask entries are 0 or 1. pair_order names every sequence exactly once; entry p is the chosen sequence of pair p and entry 8 + p the rejected one.
All inputs are finite; a program needn't handle non-finite values.
Results may differ from the reference program's by a relative error of at most 0.0015.
Values may be sent and summed in bfloat16 or wider, within the bound.
No kernel may reach another device: no remote copies, remote signals or barrier semaphores. Data moves between devices by JAX's collectives and lax.ppermute only.
A program may use at most 128 MiB of HBM per device.

```python
import jax
import jax.numpy as jnp

D = 4096
V = 128256
PAIRS = 8
SEQS = 16
LENGTH = 128


def touch_ends(entries, own_key, least, top_value):
    shape = entries.shape
    index_at = [jax.random.randint(jax.random.fold_in(own_key, axis), (), 0, shape[axis]) for axis in range(len(shape))]
    entries = entries.at[tuple(index_at)].set(least)
    longest = shape.index(max(shape))
    index_at[longest] = (index_at[longest] + 1) % shape[longest]
    return entries.at[tuple(index_at)].set(top_value)


def steps_of(key, shape, shards, low, largest):
    def one(position, parts):
        steps = jax.random.uniform(jax.random.fold_in(jax.random.fold_in(key, 6), position), (parts,), jnp.float32, low / len(shards), largest / len(shards))
        return jnp.repeat(jnp.exp(steps), shape[position] // parts).reshape((-1,) + (1,) * (len(shape) - position - 1))

    level = one(*shards[0])
    for cut in shards[1:]:
        level = level * one(*cut)
    return level


def gaussian(stream_key, dims, spread, reach, pieces=(), dtype=jnp.bfloat16):
    values = jax.random.normal(stream_key, dims, jnp.float32) * spread
    if len(pieces) > 0:
        values = steps_of(stream_key, dims, pieces, -0.22, 0.18) * values
    return jnp.clip(values, min=-reach, max=reach).astype(dtype)


def setup_inputs(seed: int = 0) -> dict:
    splits = jax.random.split(jax.random.key(seed), 7)
    hidden = gaussian(splits[0], (SEQS, LENGTH, D), 1.0, 6.0, ((1, 8), (2, 32)))
    head_weight = gaussian(splits[1], (D, V), D ** -0.5, 0.09375, ((1, 256),))
    token_ids = touch_ends(jax.random.randint(splits[2], (SEQS, LENGTH), 0, V), jax.random.fold_in(splits[2], 1), 0, V - 1).astype(jnp.int32)
    response_mask = touch_ends((jax.random.randint(splits[3], (SEQS, LENGTH), 0, 8) < 7).astype(jnp.int32), jax.random.fold_in(splits[3], 1), 0, 1)
    pair_order = jax.random.permutation(splits[4], SEQS).astype(jnp.int32)
    frozen_logprob = gaussian(splits[5], (SEQS,), 8.0, 40.0, (), jnp.float32)
    return dict(hidden=hidden, head_weight=head_weight, token_ids=token_ids, response_mask=response_mask, pair_order=pair_order, frozen_logprob=frozen_logprob)


strength = 0.1
loss_scale = 256.0


def reference(hidden, head_weight, token_ids, response_mask, pair_order, frozen_logprob):
    token_rows = hidden.reshape(SEQS * LENGTH, D)
    logits = jnp.dot(token_rows, head_weight, preferred_element_type=jnp.float32)
    row_peak = jnp.max(logits, axis=1)
    log_norm = row_peak + jnp.log(jnp.sum(jnp.exp(logits - row_peak[:, None]), axis=1))
    flat_ids = token_ids.reshape(-1).astype(jnp.int32)
    picked = jnp.take_along_axis(logits, flat_ids[:, None], axis=1)[:, 0]
    mask_flat = response_mask.reshape(-1).astype(jnp.float32)
    policy = jnp.sum(((picked - log_norm) * mask_flat).reshape(SEQS, LENGTH), axis=1)
    log_ratio = policy - frozen_logprob
    chosen = pair_order[:PAIRS]
    rejected = pair_order[PAIRS:]
    margins = strength * (log_ratio[chosen] - log_ratio[rejected])
    pair_loss = jnp.mean(jax.nn.softplus(-margins))
    weight = -loss_scale * strength * jax.nn.sigmoid(-margins) / PAIRS
    seq_coef = jnp.zeros((SEQS,), jnp.float32).at[chosen].set(weight).at[rejected].set(-weight)
    token_coef = (seq_coef[:, None] * response_mask.astype(jnp.float32)).reshape(-1)
    probabilities = jnp.exp(logits - log_norm[:, None])
    columns = jnp.arange(V).astype(jnp.int32)
    onehot = (columns[None, :] == flat_ids[:, None]).astype(jnp.float32)
    grad_logits = (token_coef[:, None] * (onehot - probabilities)).astype(jnp.bfloat16)
    spread_logits = ((V / 64.0) * token_coef[:, None] * probabilities).astype(jnp.bfloat16)
    head_grad = jnp.dot(token_rows.T, grad_logits, preferred_element_type=jnp.float32).astype(jnp.bfloat16)
    spread_grad = jnp.dot(token_rows.T, spread_logits, preferred_element_type=jnp.float32).astype(jnp.bfloat16)
    return pair_loss, margins, head_grad, spread_grad
```

```python
import jax
import jax.numpy as jnp
from jax import lax
from jax.sharding import Mesh
from jax.sharding import PartitionSpec as P

V = 128256
VOCAB = ("vocab_0", "vocab_1", "vocab_2")
CTX_VOCAB = ("ctx", "vocab_0", "vocab_1", "vocab_2")


strength = 0.1
loss_scale = 256.0


def to_planes(token_ids, response_mask):
    planes = jnp.stack([token_ids & 255, (token_ids >> 8) & 255, token_ids >> 16, response_mask])
    return planes.astype(jnp.bfloat16).reshape(-1, 128)


def from_planes(planes):
    low, mid, high, mask = planes
    ids = low.astype(jnp.int32) + 256 * mid.astype(jnp.int32) + 65536 * high.astype(jnp.int32)
    return ids, mask.astype(jnp.float32)


def exchange(lse, picked, axes, count):
    block = jnp.concatenate([lse.reshape(-1), picked, jnp.zeros((112,), jnp.float32)]).reshape(-1, 128)
    lines = lax.all_to_all(
        jnp.broadcast_to(block[None], (count, *block.shape)), axes, 0, 0, tiled=True
    )
    lines = lines.reshape(count, -1)
    parts = lines[:, : lse.size]
    peak = jnp.max(parts, axis=0)
    total = peak + jnp.log(jnp.sum(jnp.exp(parts - peak), axis=0))
    return total, jnp.sum(lines[:, lse.size : lse.size + picked.size], axis=0)


def contract_rows(block_rows, both_logits):
    return lax.dot_general(
        block_rows, both_logits, (((0,), (0,)), ((), ())), preferred_element_type=jnp.float32
    )


def shards(hidden, head_weight, token_ids, response_mask, pair_order, frozen_logprob):
    seqs, local, width = hidden.shape
    rows = seqs * local
    block = jnp.concatenate([hidden.reshape(rows, width), to_planes(token_ids, response_mask)])
    blocks = lax.all_gather(block, "ctx", axis=0)
    ctx_count = blocks.shape[0]
    token_rows = blocks[:, :rows].reshape(ctx_count * rows, width)
    planes = blocks[:, rows:].reshape(ctx_count, 4, rows)
    ids_flat, mask_flat = from_planes(jnp.moveaxis(planes, 1, 0).reshape(4, -1))
    shard_width = head_weight.shape[1]
    whole_rows = lax.all_gather(token_rows, VOCAB, axis=1, tiled=True)
    logits = jnp.dot(whole_rows, head_weight, preferred_element_type=jnp.float32)
    offset = lax.axis_index(CTX_VOCAB) * shard_width
    local_ids = ids_flat - offset
    columns = jnp.arange(shard_width).astype(jnp.int32)
    hit = columns[None, :] == local_ids[:, None]
    picked_part = jnp.sum(jnp.where(hit, logits, 0.0), axis=1)
    peak = jnp.max(logits, axis=1)
    lse = peak + jnp.log(jnp.sum(jnp.exp(logits - peak[:, None]), axis=1))
    by_seq = (picked_part * mask_flat).reshape(ctx_count, seqs, local).sum(axis=(0, 2))
    lse, by_seq = exchange(lse, by_seq, VOCAB, 32)
    log_norm, picked = exchange(lse, by_seq, "ctx", ctx_count)
    norm_seq = (log_norm * mask_flat).reshape(ctx_count, seqs, local).sum(axis=(0, 2))
    policy = picked - norm_seq
    log_ratio = policy - frozen_logprob
    pair_count = pair_order.shape[0] // 2
    seq_ids = jnp.arange(seqs)
    is_chosen = (pair_order[:pair_count, None] == seq_ids[None, :]).astype(jnp.float32)
    is_rejected = (pair_order[pair_count:, None] == seq_ids[None, :]).astype(jnp.float32)
    margins = strength * (
        jnp.sum(is_chosen * log_ratio[None], axis=1) - jnp.sum(is_rejected * log_ratio[None], axis=1)
    )
    pair_loss = jnp.mean(jax.nn.softplus(-margins))
    weight = -loss_scale * strength * jax.nn.sigmoid(-margins) / pair_count
    seq_coef = jnp.sum(weight[:, None] * (is_chosen - is_rejected), axis=0)
    token_coef = mask_flat * jnp.broadcast_to(
        seq_coef[None, :, None], (ctx_count, seqs, local)
    ).reshape(-1)
    probabilities = jnp.exp(logits - log_norm[:, None])
    onehot = hit.astype(jnp.float32)
    grad_logits = (token_coef[:, None] * (onehot - probabilities)).astype(jnp.bfloat16)
    spread_logits = (V / 64.0 * token_coef[:, None] * probabilities).astype(jnp.bfloat16)
    both_logits = jnp.concatenate([grad_logits, spread_logits], axis=1)
    both_grads = contract_rows(whole_rows, both_logits)
    head_grad = both_grads[:, :shard_width].astype(jnp.bfloat16)
    spread_grad = both_grads[:, shard_width:].astype(jnp.bfloat16)
    return (pair_loss, margins, head_grad, spread_grad)


def solution(mesh):
    split = Mesh(
        mesh.devices.reshape(mesh.shape["ctx"], 4, 4, 2), ("ctx", "vocab_0", "vocab_1", "vocab_2")
    )
    placed = (P(None, "ctx", VOCAB), P(None, CTX_VOCAB), P(None, "ctx"), P(None, "ctx"), P(), P())
    return jax.shard_map(
        shards,
        mesh=split,
        in_specs=placed,
        out_specs=(P(), P(), P(None, CTX_VOCAB), P(None, CTX_VOCAB)),
        check_vma=False,
    )
```

```python
import functools

import jax
import jax.numpy as jnp
from jax import lax
from jax.experimental import pallas as pl
from jax.experimental.pallas import tpu as pltpu
from jax.sharding import Mesh
from jax.sharding import PartitionSpec as P

V = 128256
VOCAB = ("vocab_0", "vocab_1", "vocab_2")
CTX_VOCAB = ("ctx", "vocab_0", "vocab_1", "vocab_2")

strength = 0.1
loss_scale = 256.0

ROWS = 1024
UNIT = 256
CHUNK = 256
FIRST, LAST = (0, -1), (1, 2)
EARLY = tuple(tuple((d1, d2) for d1 in pair) for d2 in (0, -1, 1) for pair in (FIRST, LAST))
LATE = tuple(tuple((d1, 2) for d1 in pair) for pair in (FIRST, LAST))
VMEM_LIMIT = 60 * 1024 * 1024


def to_planes(token_ids, response_mask):
    planes = jnp.stack([token_ids & 255, (token_ids >> 8) & 255, token_ids >> 16, response_mask])
    return planes.astype(jnp.bfloat16).reshape(4, -1)


def from_planes(planes):
    low, mid, high, mask = planes
    ids = low.astype(jnp.int32) + 256 * mid.astype(jnp.int32) + 65536 * high.astype(jnp.int32)
    return ids, mask.astype(jnp.float32)


def shift(value, axis, step, size):
    return lax.ppermute(value, axis, [(i, (i + step) % size) for i in range(size)])


def colour_pairs(second, step):
    pairs = []
    for y in range(4):
        for x in range(4):
            for core in range(2):
                along_x = (core == 0) != second
                to_y, to_x = (y, (x + step) % 4) if along_x else ((y + step) % 4, x)
                pairs.append(((y * 4 + x) * 2 + core, (to_y * 4 + to_x) * 2 + core))
    return pairs


def exchange(lse, picked, axes, count):
    block = jnp.concatenate([lse.reshape(-1), picked, jnp.zeros((112,), jnp.float32)]).reshape(-1, 128)
    lines = lax.all_to_all(
        jnp.broadcast_to(block[None], (count, *block.shape)), axes, 0, 0, tiled=True
    )
    lines = lines.reshape(count, -1)
    parts = lines[:, : lse.size]
    peak = jnp.max(parts, axis=0)
    total = peak + jnp.log(jnp.sum(jnp.exp(parts - peak), axis=0))
    return total, jnp.sum(lines[:, lse.size : lse.size + picked.size], axis=0)


def spread_over(block):
    first = lambda value, step: lax.ppermute(value, VOCAB, colour_pairs(False, step))
    second = lambda value, step: lax.ppermute(value, VOCAB, colour_pairs(True, step))
    below = first(block, 1)
    above = first(block, -1)
    far = first(below, 1)
    head = jnp.concatenate([block, below])
    head_below, head_above = second(head, 1), second(head, -1)
    rest = jnp.concatenate([above, far])
    rest_below, rest_above = second(rest, 1), second(rest, -1)
    late = [second(head_above, -1), second(rest_below, 1)]
    return [head, rest, head_below, rest_below, head_above, rest_above], late


def chip_of(pos_ref, offset, colour):
    d1, d2 = offset
    y = (pos_ref[0] + (d2 + 4) + colour * (d1 - d2)) & 3
    x = (pos_ref[1] + (d1 + 4) + colour * (d2 - d1)) & 3
    return y * 4 + x


def logits_kernel(offsets, late, *refs):
    pos_ref, refs = refs[0], refs[1:]
    count = len(offsets)
    sources, refs = (refs[:count], refs[count : 2 * count]), refs[2 * count :]
    weight, refs = refs[0], refs[1:]
    if late:
        partial, ids_ref, out, lse_ref, picked_ref, lhs, rhs, acc, sem_l, sem_r, sem_p, sem_o = refs
    else:
        out, lhs, rhs, acc, sem_l, sem_r, sem_o = refs
    steps = ROWS // CHUNK
    colours = (pos_ref[2], 1 - pos_ref[2])

    def columns(half, i):
        return pl.ds(pl.multiple_of(colours[half] * ROWS + i * CHUNK, CHUNK), CHUNK)

    for half in range(2):
        slot = 0
        for source, blocks in zip(sources[half], offsets):
            for j, offset in enumerate(blocks):
                pltpu.make_async_copy(
                    source.at[pl.ds(j * ROWS, ROWS), :],
                    rhs.at[half, :, pl.ds(slot * UNIT, UNIT)],
                    sem_r.at[half],
                ).start()
                chip = chip_of(pos_ref, offset, colours[half])
                pltpu.make_async_copy(
                    weight.at[:, pl.ds(pl.multiple_of(chip * UNIT, UNIT), UNIT)],
                    lhs.at[half, :, pl.ds(slot * UNIT, UNIT)],
                    sem_l.at[half],
                ).start()
                slot += 1
        if late:
            for i in range(steps):
                pltpu.make_async_copy(partial.at[:, columns(half, i)], acc.at[half, i], sem_p.at[half, i]).start()
    for half in range(2):
        pltpu.make_async_copy(rhs.at[half], rhs.at[half], sem_r.at[half]).wait()
        pltpu.make_async_copy(lhs.at[half], lhs.at[half], sem_l.at[half]).wait()

        def step(i, carry):
            rows = pl.ds(pl.multiple_of(i * CHUNK, CHUNK), CHUNK)
            got = lax.dot_general(
                lhs[half], rhs[half, rows, :], (((1,), (1,)), ((), ())), preferred_element_type=jnp.float32
            )
            if late:
                pltpu.make_async_copy(partial.at[:, columns(half, i)], acc.at[half, i], sem_p.at[half, i]).wait()
                got = got + acc[half, i]
                line = pl.ds(colours[half] * steps + i, 1)
                peak = jnp.max(got, axis=0, keepdims=True)
                lse_ref[line, :] = peak + jnp.log(jnp.sum(jnp.exp(got - peak), axis=0, keepdims=True))
                here = lax.broadcasted_iota(jnp.int32, got.shape, 0) == ids_ref[line, :]
                picked_ref[line, :] = jnp.sum(jnp.where(here, got, 0.0), axis=0, keepdims=True)
            acc[half, i] = got
            pltpu.make_async_copy(acc.at[half, i], out.at[:, columns(half, i)], sem_o.at[half, i]).start()
            return carry

        lax.fori_loop(0, steps, step, 0)
    for half in range(2):
        for i in range(steps):
            pltpu.make_async_copy(acc.at[half, i], out.at[:, columns(half, i)], sem_o.at[half, i]).wait()


def logits_call(offsets, position, own, other, weight, partial=None, ids=None):
    late = partial is not None
    depth = sum(map(len, offsets)) * UNIT
    width = weight.shape[0]
    steps = ROWS // CHUNK
    hbm = pl.BlockSpec(memory_space=pltpu.HBM)
    vmem = pl.BlockSpec(memory_space=pltpu.VMEM)
    operands = [position, *own, *other, weight] + ([partial] if late else [])
    in_specs = [pl.BlockSpec(memory_space=pltpu.SMEM)] + [hbm] * (len(operands) - 1)
    outs, out_specs = [jax.ShapeDtypeStruct((width, 2 * ROWS), jnp.float32)], [hbm]
    if late:
        operands, in_specs = operands + [ids], in_specs + [vmem]
        outs, out_specs = outs + [jax.ShapeDtypeStruct((2 * steps, CHUNK), jnp.float32)] * 2, out_specs + [vmem] * 2
    return pl.pallas_call(
        functools.partial(logits_kernel, offsets, late),
        out_shape=tuple(outs),
        in_specs=in_specs,
        out_specs=tuple(out_specs),
        scratch_shapes=[
            pltpu.VMEM((2, width, depth), jnp.bfloat16),
            pltpu.VMEM((2, ROWS, depth), jnp.bfloat16),
            pltpu.VMEM((2, steps, width, CHUNK), jnp.float32),
            pltpu.SemaphoreType.DMA((2,)),
            pltpu.SemaphoreType.DMA((2,)),
        ]
        + [pltpu.SemaphoreType.DMA((2, steps))] * (2 if late else 1),
        compiler_params=pltpu.CompilerParams(vmem_limit_bytes=VMEM_LIMIT),
        cost_estimate=pl.CostEstimate(
            flops=4 * ROWS * depth * width, bytes_accessed=4 * ROWS * depth, transcendentals=0
        ),
        name="logits_late" if late else "logits_early",
    )(*operands)


PAD = 512


def grads_kernel(*refs):
    pos_ref, refs = refs[0], refs[1:]
    offsets = EARLY + LATE
    count = len(offsets)
    sources, refs = (refs[:count], refs[count : 2 * count]), refs[2 * count :]
    logits, norm_ref, coef_ref, ids_ref, out_g, out_s, rhs, both, stage, sem_r, sem_o = refs
    width = logits.shape[0]
    colours = (pos_ref[2], 1 - pos_ref[2])
    place = {
        (d1 & 3, d2 & 3): (n, j) for n, blocks in enumerate(offsets) for j, (d1, d2) in enumerate(blocks)
    }
    for unit in range(16):
        d1, d2 = unit // 4, unit % 4
        for half, offset in enumerate(((d1, d2), (d2, d1))):
            n, j = place[offset]
            at = pl.multiple_of(colours[half] * ROWS, ROWS)
            pltpu.make_async_copy(
                sources[half][n].at[pl.ds(j * ROWS, ROWS), :], rhs.at[unit, pl.ds(at, ROWS), :], sem_r.at[unit]
            ).start()

    both[pl.ds(width // 8 * 8, PAD - width // 8 * 8), :] = jnp.zeros((PAD - width // 8 * 8, 2 * ROWS), jnp.bfloat16)
    tail = PAD + width // 8 * 8
    both[pl.ds(tail, 2 * PAD - tail), :] = jnp.zeros((2 * PAD - tail, 2 * ROWS), jnp.bfloat16)
    for i in range(2 * ROWS // CHUNK):
        rows = pl.ds(i * CHUNK, CHUNK)
        chance = jnp.exp(logits[:, rows] - norm_ref[pl.ds(i, 1), :])
        coef = coef_ref[pl.ds(i, 1), :]
        here = lax.broadcasted_iota(jnp.int32, chance.shape, 0) == ids_ref[pl.ds(i, 1), :]
        both[pl.ds(0, width), rows] = (coef * (jnp.where(here, 1.0, 0.0) - chance)).astype(jnp.bfloat16)
        both[pl.ds(PAD, width), rows] = ((V / 64.0) * coef * chance).astype(jnp.bfloat16)

    def outputs(unit):
        slot = unit & 1
        chip = chip_of(pos_ref, (unit >> 2, unit & 3), colours[0])
        at = pl.ds(pl.multiple_of(chip * UNIT, UNIT), UNIT)
        return [
            pltpu.make_async_copy(stage.at[slot, n], out.at[:, at], sem_o.at[slot, n])
            for n, out in enumerate((out_g, out_s))
        ]

    def one(unit, carry):
        pltpu.make_async_copy(rhs.at[unit], rhs.at[unit], sem_r.at[unit]).wait()

        @pl.when(unit >= 2)
        def _():
            for copy in outputs(unit - 2):
                copy.wait()

        got = jnp.dot(both[...], rhs[unit], preferred_element_type=jnp.float32)
        stage[unit & 1, 0] = got[:width].astype(jnp.bfloat16)
        stage[unit & 1, 1] = got[PAD : PAD + width].astype(jnp.bfloat16)
        for copy in outputs(unit):
            copy.start()
        return carry

    lax.fori_loop(0, 16, one, 0)
    for unit in (14, 15):
        for copy in outputs(unit):
            copy.wait()


def grads_call(position, own, other, logits, norm, coef, ids):
    width = logits.shape[0]
    features = 16 * UNIT
    hbm = pl.BlockSpec(memory_space=pltpu.HBM)
    vmem = pl.BlockSpec(memory_space=pltpu.VMEM)
    out = jax.ShapeDtypeStruct((width, features), jnp.bfloat16)
    return pl.pallas_call(
        grads_kernel,
        out_shape=(out, out),
        in_specs=[pl.BlockSpec(memory_space=pltpu.SMEM)] + [hbm] * (2 * len(own)) + [vmem] * 4,
        out_specs=(hbm, hbm),
        scratch_shapes=[
            pltpu.VMEM((16, 2 * ROWS, UNIT), jnp.bfloat16),
            pltpu.VMEM((2 * PAD, 2 * ROWS), jnp.bfloat16),
            pltpu.VMEM((2, 2, width, UNIT), jnp.bfloat16),
            pltpu.SemaphoreType.DMA((16,)),
            pltpu.SemaphoreType.DMA((2, 2)),
        ],
        compiler_params=pltpu.CompilerParams(vmem_limit_bytes=VMEM_LIMIT),
        cost_estimate=pl.CostEstimate(
            flops=8 * ROWS * features * width, bytes_accessed=4 * ROWS * features, transcendentals=0
        ),
        name="head_grads",
    )(position, *own, *other, logits, norm, coef, ids)


def shards(hidden, head_weight, token_ids, response_mask, pair_order, frozen_logprob):
    seqs, local, width = hidden.shape
    rows = seqs * local
    part = rows // 2
    ctx_count = 8
    y, x, core = (lax.axis_index(axis) for axis in VOCAB)
    position = jnp.stack([y, x, core]).astype(jnp.int32)
    flat = hidden.reshape(rows, width)
    low, high = flat[:part], flat[part:]
    mine, theirs = jnp.where(core == 0, low, high), jnp.where(core == 0, high, low)
    swapped = shift(theirs, "vocab_2", 1, 2)
    colour_rows = jnp.where(
        core == 0, jnp.concatenate([mine, swapped], axis=1), jnp.concatenate([swapped, mine], axis=1)
    )
    planes = to_planes(token_ids, response_mask)
    block = jnp.concatenate([colour_rows, planes, jnp.zeros_like(planes)])
    blocks = [block] + [shift(block, "ctx", k, ctx_count) for k in range(1, ctx_count)]
    planes = jnp.stack([b[part : part + 4].reshape(4, 2, part) for b in blocks], axis=2)
    ids, mask = from_planes(planes)
    early, late = spread_over(jnp.concatenate([b[:part] for b in blocks]))
    early_other = [shift(piece, "vocab_2", 1, 2) for piece in early]
    late_other = [shift(piece, "vocab_2", 1, 2) for piece in late]
    shard_width = head_weight.shape[1]
    lines = (2 * ROWS // CHUNK, CHUNK)
    local_ids = (ids - lax.axis_index(CTX_VOCAB) * shard_width).reshape(lines)
    weight_t = head_weight.T
    (partial,) = logits_call(EARLY, position, early, early_other, weight_t)
    logits, lse, picked = logits_call(LATE, position, late, late_other, weight_t, partial, local_ids)

    per_seq = (2, ctx_count, seqs // 2, local)
    by_seq = jnp.sum((picked.reshape(per_seq) * mask.reshape(per_seq)), axis=(1, 3)).reshape(-1)
    lse, by_seq = exchange(lse, by_seq, VOCAB, 32)
    turn = (lax.axis_index("ctx") - jnp.arange(ctx_count)) % ctx_count
    log_norm, picked = exchange(lse.reshape(2, ctx_count, part)[:, turn], by_seq, "ctx", ctx_count)
    norm_seq = jnp.sum(log_norm.reshape(per_seq) * mask[:, turn].reshape(per_seq), axis=(1, 3)).reshape(-1)
    log_norm = log_norm.reshape(2, ctx_count, part)[:, turn]
    policy = picked - norm_seq
    log_ratio = policy - frozen_logprob
    pair_count = pair_order.shape[0] // 2
    seq_ids = jnp.arange(seqs)
    is_chosen = (pair_order[:pair_count, None] == seq_ids[None, :]).astype(jnp.float32)
    is_rejected = (pair_order[pair_count:, None] == seq_ids[None, :]).astype(jnp.float32)
    margins = strength * (
        jnp.sum(is_chosen * log_ratio[None], axis=1) - jnp.sum(is_rejected * log_ratio[None], axis=1)
    )
    pair_loss = jnp.mean(jax.nn.softplus(-margins))
    weight = -loss_scale * strength * jax.nn.sigmoid(-margins) / pair_count
    seq_coef = jnp.sum(weight[:, None] * (is_chosen - is_rejected), axis=0)
    token_coef = mask.reshape(per_seq) * seq_coef.reshape(2, 1, seqs // 2, 1)
    head_grad, spread_grad = grads_call(
        position, early + late, early_other + late_other, logits,
        log_norm.reshape(lines), token_coef.reshape(lines), local_ids,
    )
    return (pair_loss, margins, head_grad.T, spread_grad.T)


def solution(mesh):
    split = Mesh(
        mesh.devices.reshape(mesh.shape["ctx"], 4, 4, 2), ("ctx", "vocab_0", "vocab_1", "vocab_2")
    )
    placed = (P(None, "ctx", VOCAB), P(None, CTX_VOCAB), P(None, "ctx"), P(None, "ctx"), P(), P())
    return jax.shard_map(
        shards,
        mesh=split,
        in_specs=placed,
        out_specs=(P(), P(), P(None, CTX_VOCAB), P(None, CTX_VOCAB)),
        check_vma=False,
    )
```

```python
import functools

import jax
import jax.numpy as jnp
from jax import lax
from jax.experimental import pallas as pl
from jax.experimental.pallas import tpu as pltpu
from jax.sharding import Mesh
from jax.sharding import PartitionSpec as P


V = 128256
VOCAB = ("vocab_0", "vocab_1", "vocab_2")
CTX_VOCAB = ("ctx", "vocab_0", "vocab_1", "vocab_2")

strength = 0.1
loss_scale = 256.0

ROWS = 1024
UNIT = 256
CHUNK = 256
FIRST, LAST = (0, -1), (1, 2)
EARLY = tuple(tuple((d1, d2) for d1 in pair) for d2, pair in ((0, FIRST), (0, LAST), (-1, FIRST), (1, FIRST)))
LATE = tuple(tuple((d1, d2) for d1 in pair) for d2, pair in ((-1, LAST), (1, LAST), (2, FIRST), (2, LAST)))
VMEM_LIMIT = 60 * 1024 * 1024


def to_planes(token_ids, response_mask):
    planes = jnp.stack([token_ids & 255, (token_ids >> 8) & 255, token_ids >> 16, response_mask])
    return planes.astype(jnp.bfloat16).reshape(4, -1)


def from_planes(planes):
    low, mid, high, mask = planes
    ids = low.astype(jnp.int32) + 256 * mid.astype(jnp.int32) + 65536 * high.astype(jnp.int32)
    return ids, mask.astype(jnp.float32)


def shift(value, axis, step, size):
    return lax.ppermute(value, axis, [(i, (i + step) % size) for i in range(size)])


def swap(value):
    return shift(value, "vocab_2", 1, 2)


def colour_pairs(second, step):
    pairs = []
    for y in range(4):
        for x in range(4):
            for core in range(2):
                along_x = (core == 0) != second
                to_y, to_x = (y, (x + step) % 4) if along_x else ((y + step) % 4, x)
                pairs.append(((y * 4 + x) * 2 + core, (to_y * 4 + to_x) * 2 + core))
    return pairs


def exchange(lse, picked, axes, count):
    block = jnp.concatenate([lse.reshape(-1), picked, jnp.zeros((112,), jnp.float32)]).reshape(-1, 128)
    lines = lax.all_to_all(
        jnp.broadcast_to(block[None], (count, *block.shape)), axes, 0, 0, tiled=True
    )
    lines = lines.reshape(count, -1)
    parts = lines[:, : lse.size]
    peak = jnp.max(parts, axis=0)
    total = peak + jnp.log(jnp.sum(jnp.exp(parts - peak), axis=0))
    return total, jnp.sum(lines[:, lse.size : lse.size + picked.size], axis=0)


def spread_over(block):
    def first(value, step):
        return lax.ppermute(value, VOCAB, colour_pairs(False, step))

    def second(value, step):
        return lax.ppermute(value, VOCAB, colour_pairs(True, step))

    below = first(block, 1)
    above = first(block, -1)
    head = jnp.concatenate([block, below])
    head_above = second(head, -1)
    head_below = second(head, 1)
    far = first(below, 1)
    rest = jnp.concatenate([above, far])
    rest_below, rest_above = second(rest, 1), second(rest, -1)
    across = [second(head_above, -1), second(rest_below, 1)]
    return [head, rest, head_below, head_above], [rest_below, rest_above, *across]


def chip_of(pos_ref, offset, colour):
    d1, d2 = offset
    y = (pos_ref[0] + (d2 + 4) + colour * (d1 - d2)) & 3
    x = (pos_ref[1] + (d1 + 4) + colour * (d2 - d1)) & 3
    return y * 4 + x


def logits_kernel(offsets, late, *refs):
    pos_ref, refs = refs[0], refs[1:]
    count = len(offsets)
    sources, refs = (refs[:count], refs[count : 2 * count]), refs[2 * count :]
    weight, refs = refs[0], refs[1:]
    if late:
        partial, ids_ref, out, lse_ref, picked_ref, lhs, rhs, acc, sem_l, sem_r, sem_p, sem_o = refs
    else:
        out, lhs, rhs, acc, sem_l, sem_r, sem_o = refs
    steps = ROWS // CHUNK
    colours = (pos_ref[2], 1 - pos_ref[2])

    def columns(half, i):
        return pl.ds(pl.multiple_of(colours[half] * ROWS + i * CHUNK, CHUNK), CHUNK)

    for half in range(2):
        slots = [(n, j, offset) for n, blocks in enumerate(offsets) for j, offset in enumerate(blocks)]
        for slot, (n, j, offset) in enumerate(slots):
            chip = chip_of(pos_ref, offset, colours[half])
            pltpu.make_async_copy(
                weight.at[:, pl.ds(pl.multiple_of(chip * UNIT, UNIT), UNIT)],
                lhs.at[half, :, pl.ds(slot * UNIT, UNIT)],
                sem_l.at[half],
            ).start()
        for i in range(steps):
            for slot, (n, j, offset) in enumerate(slots):
                pltpu.make_async_copy(
                    sources[half][n].at[pl.ds(j * ROWS + i * CHUNK, CHUNK), :],
                    rhs.at[half, i, :, pl.ds(slot * UNIT, UNIT)],
                    sem_r.at[half, i],
                ).start()
            if late:
                pltpu.make_async_copy(partial.at[:, columns(half, i)], acc.at[half, i], sem_p.at[half, i]).start()
    for half in range(2):
        pltpu.make_async_copy(lhs.at[half], lhs.at[half], sem_l.at[half]).wait()

        def step(pair, carry):
            chunks = (2 * pair, 2 * pair + 1)
            for i in chunks:
                pltpu.make_async_copy(rhs.at[half, i], rhs.at[half, i], sem_r.at[half, i]).wait()
                if late:
                    pltpu.make_async_copy(partial.at[:, columns(half, i)], acc.at[half, i], sem_p.at[half, i]).wait()
            for i in chunks:
                got = lax.dot_general(
                    lhs[half], rhs[half, i], (((1,), (1,)), ((), ())), preferred_element_type=jnp.float32
                )
                if late:
                    got = got + acc[half, i]
                    line = pl.ds(colours[half] * steps + i, 1)
                    peak = jnp.max(got, axis=0, keepdims=True)
                    lse_ref[line, :] = peak + jnp.log(jnp.sum(jnp.exp(got - peak), axis=0, keepdims=True))
                    here = lax.broadcasted_iota(jnp.int32, got.shape, 0) == ids_ref[line, :]
                    picked_ref[line, :] = jnp.sum(jnp.where(here, got, 0.0), axis=0, keepdims=True)
                acc[half, i] = got
            for i in chunks:
                pltpu.make_async_copy(acc.at[half, i], out.at[:, columns(half, i)], sem_o.at[half, i]).start()
            return carry

        lax.fori_loop(0, steps // 2, step, 0)
    for half in range(2):
        for i in range(steps):
            pltpu.make_async_copy(acc.at[half, i], out.at[:, columns(half, i)], sem_o.at[half, i]).wait()


def logits_call(offsets, position, own, other, weight, partial=None, ids=None):
    late = partial is not None
    depth = sum(map(len, offsets)) * UNIT
    width = weight.shape[0]
    steps = ROWS // CHUNK
    hbm = pl.BlockSpec(memory_space=pltpu.HBM)
    vmem = pl.BlockSpec(memory_space=pltpu.VMEM)
    operands = [position, *own, *other, weight] + ([partial] if late else [])
    in_specs = [pl.BlockSpec(memory_space=pltpu.SMEM)] + [hbm] * (len(operands) - 1)
    outs, out_specs = [jax.ShapeDtypeStruct((width, 2 * ROWS), jnp.float32)], [hbm]
    if late:
        operands, in_specs = operands + [ids], in_specs + [vmem]
        outs, out_specs = outs + [jax.ShapeDtypeStruct((2 * steps, CHUNK), jnp.float32)] * 2, out_specs + [vmem] * 2
    return pl.pallas_call(
        functools.partial(logits_kernel, offsets, late),
        out_shape=tuple(outs),
        in_specs=in_specs,
        out_specs=tuple(out_specs),
        scratch_shapes=[
            pltpu.VMEM((2, width, depth), jnp.bfloat16),
            pltpu.VMEM((2, steps, CHUNK, depth), jnp.bfloat16),
            pltpu.VMEM((2, steps, width, CHUNK), jnp.float32),
            pltpu.SemaphoreType.DMA((2,)),
        ]
        + [pltpu.SemaphoreType.DMA((2, steps))] * (3 if late else 2),
        compiler_params=pltpu.CompilerParams(vmem_limit_bytes=VMEM_LIMIT),
        cost_estimate=pl.CostEstimate(
            flops=4 * ROWS * depth * width, bytes_accessed=4 * ROWS * depth, transcendentals=0
        ),
        name="logits_late" if late else "logits_early",
    )(*operands)


PAD = 512


def grads_kernel(*refs):
    pos_ref, refs = refs[0], refs[1:]
    offsets = EARLY + LATE
    count = len(offsets)
    sources, refs = (refs[:count], refs[count : 2 * count]), refs[2 * count :]
    logits, norm_ref, coef_ref, ids_ref, out_g, out_s, rhs, both, stage, sem_r, sem_o = refs
    width = logits.shape[0]
    colours = (pos_ref[2], 1 - pos_ref[2])
    place = {
        (d1 & 3, d2 & 3): (n, j) for n, blocks in enumerate(offsets) for j, (d1, d2) in enumerate(blocks)
    }
    for unit in range(16):
        d1, d2 = unit // 4, unit % 4
        for half, offset in enumerate(((d1, d2), (d2, d1))):
            n, j = place[offset]
            at = pl.multiple_of(colours[half] * ROWS, ROWS)
            pltpu.make_async_copy(
                sources[half][n].at[pl.ds(j * ROWS, ROWS), :], rhs.at[unit, pl.ds(at, ROWS), :], sem_r.at[unit]
            ).start()

    both[pl.ds(width // 8 * 8, PAD - width // 8 * 8), :] = jnp.zeros((PAD - width // 8 * 8, 2 * ROWS), jnp.bfloat16)
    tail = PAD + width // 8 * 8
    both[pl.ds(tail, 2 * PAD - tail), :] = jnp.zeros((2 * PAD - tail, 2 * ROWS), jnp.bfloat16)
    for i in range(2 * ROWS // CHUNK):
        rows = pl.ds(i * CHUNK, CHUNK)
        chance = jnp.exp(logits[:, rows] - norm_ref[pl.ds(i, 1), :])
        coef = coef_ref[pl.ds(i, 1), :]
        here = lax.broadcasted_iota(jnp.int32, chance.shape, 0) == ids_ref[pl.ds(i, 1), :]
        both[pl.ds(0, width), rows] = (coef * (jnp.where(here, 1.0, 0.0) - chance)).astype(jnp.bfloat16)
        both[pl.ds(PAD, width), rows] = ((V / 64.0) * coef * chance).astype(jnp.bfloat16)

    def outputs(unit):
        slot = unit & 1
        chip = chip_of(pos_ref, (unit >> 2, unit & 3), colours[0])
        at = pl.ds(pl.multiple_of(chip * UNIT, UNIT), UNIT)
        return [
            pltpu.make_async_copy(stage.at[slot, n], out.at[:, at], sem_o.at[slot, n])
            for n, out in enumerate((out_g, out_s))
        ]

    def one(unit, carry):
        pltpu.make_async_copy(rhs.at[unit], rhs.at[unit], sem_r.at[unit]).wait()

        @pl.when(unit >= 2)
        def _():
            for copy in outputs(unit - 2):
                copy.wait()

        got = jnp.dot(both[...], rhs[unit], preferred_element_type=jnp.float32)
        stage[unit & 1, 0] = got[:width].astype(jnp.bfloat16)
        stage[unit & 1, 1] = got[PAD : PAD + width].astype(jnp.bfloat16)
        for copy in outputs(unit):
            copy.start()
        return carry

    lax.fori_loop(0, 16, one, 0)
    for unit in (14, 15):
        for copy in outputs(unit):
            copy.wait()


def grads_call(position, own, other, logits, norm, coef, ids):
    width = logits.shape[0]
    features = 16 * UNIT
    hbm = pl.BlockSpec(memory_space=pltpu.HBM)
    vmem = pl.BlockSpec(memory_space=pltpu.VMEM)
    out = jax.ShapeDtypeStruct((width, features), jnp.bfloat16)
    return pl.pallas_call(
        grads_kernel,
        out_shape=(out, out),
        in_specs=[pl.BlockSpec(memory_space=pltpu.SMEM)] + [hbm] * (2 * len(own)) + [vmem] * 4,
        out_specs=(hbm, hbm),
        scratch_shapes=[
            pltpu.VMEM((16, 2 * ROWS, UNIT), jnp.bfloat16),
            pltpu.VMEM((2 * PAD, 2 * ROWS), jnp.bfloat16),
            pltpu.VMEM((2, 2, width, UNIT), jnp.bfloat16),
            pltpu.SemaphoreType.DMA((16,)),
            pltpu.SemaphoreType.DMA((2, 2)),
        ],
        compiler_params=pltpu.CompilerParams(vmem_limit_bytes=VMEM_LIMIT),
        cost_estimate=pl.CostEstimate(
            flops=8 * ROWS * features * width, bytes_accessed=4 * ROWS * features, transcendentals=0
        ),
        name="head_grads",
    )(position, *own, *other, logits, norm, coef, ids)


def shards_body(hidden, head_weight, token_ids, response_mask, pair_order, frozen_logprob):
    seqs, local, width = hidden.shape
    rows = seqs * local
    part = rows // 2
    ctx_count = 8
    y, x, core = (lax.axis_index(axis) for axis in VOCAB)
    position = jnp.stack([y, x, core]).astype(jnp.int32)
    flat = hidden.reshape(rows, width)
    low, high = flat[:part], flat[part:]
    mine, theirs = jnp.where(core == 0, low, high), jnp.where(core == 0, high, low)
    swapped = shift(theirs, "vocab_2", 1, 2)
    colour_rows = jnp.where(
        core == 0, jnp.concatenate([mine, swapped], axis=1), jnp.concatenate([swapped, mine], axis=1)
    )
    planes = to_planes(token_ids, response_mask)
    block = jnp.concatenate([colour_rows, planes, jnp.zeros_like(planes)])
    blocks = [block] + [shift(block, "ctx", k, ctx_count) for k in range(1, ctx_count)]
    planes = jnp.stack([b[part : part + 4].reshape(4, 2, part) for b in blocks], axis=2)
    ids, mask = from_planes(planes)
    early, late = spread_over(jnp.concatenate([b[:part] for b in blocks]))
    early_other = [swap(piece) for piece in early]
    late_other = [swap(piece) for piece in late]
    shard_width = head_weight.shape[1]
    lines = (2 * ROWS // CHUNK, CHUNK)
    local_ids = (ids - lax.axis_index(CTX_VOCAB) * shard_width).reshape(lines)
    weight_t = head_weight.T
    (partial,) = logits_call(EARLY, position, early, early_other, weight_t)
    logits, lse, picked = logits_call(LATE, position, late, late_other, weight_t, partial, local_ids)

    per_seq = (2, ctx_count, seqs // 2, local)
    by_seq = jnp.sum((picked.reshape(per_seq) * mask.reshape(per_seq)), axis=(1, 3)).reshape(-1)
    lse, by_seq = exchange(lse, by_seq, VOCAB, 32)
    turn = (lax.axis_index("ctx") - jnp.arange(ctx_count)) % ctx_count
    log_norm, picked = exchange(lse.reshape(2, ctx_count, part)[:, turn], by_seq, "ctx", ctx_count)
    norm_seq = jnp.sum(log_norm.reshape(per_seq) * mask[:, turn].reshape(per_seq), axis=(1, 3)).reshape(-1)
    log_norm = log_norm.reshape(2, ctx_count, part)[:, turn]
    policy = picked - norm_seq
    log_ratio = policy - frozen_logprob
    pair_count = pair_order.shape[0] // 2
    seq_ids = jnp.arange(seqs)
    is_chosen = (pair_order[:pair_count, None] == seq_ids[None, :]).astype(jnp.float32)
    is_rejected = (pair_order[pair_count:, None] == seq_ids[None, :]).astype(jnp.float32)
    margins = strength * (
        jnp.sum(is_chosen * log_ratio[None], axis=1) - jnp.sum(is_rejected * log_ratio[None], axis=1)
    )
    pair_loss = jnp.mean(jax.nn.softplus(-margins))
    weight = -loss_scale * strength * jax.nn.sigmoid(-margins) / pair_count
    seq_coef = jnp.sum(weight[:, None] * (is_chosen - is_rejected), axis=0)
    token_coef = mask.reshape(per_seq) * seq_coef.reshape(2, 1, seqs // 2, 1)
    head_grad, spread_grad = grads_call(
        position, early + late, early_other + late_other, logits,
        log_norm.reshape(lines), token_coef.reshape(lines), local_ids,
    )
    return (pair_loss, margins, head_grad.T, spread_grad.T)


def solution(mesh):
    split = Mesh(
        mesh.devices.reshape(mesh.shape["ctx"], 4, 4, 2), ("ctx", "vocab_0", "vocab_1", "vocab_2")
    )
    placed = (P(None, "ctx", VOCAB), P(None, CTX_VOCAB), P(None, "ctx"), P(None, "ctx"), P(), P())
    return jax.shard_map(
        shards_body,
        mesh=split,
        in_specs=placed,
        out_specs=(P(), P(), P(None, CTX_VOCAB), P(None, CTX_VOCAB)),
        check_vma=False,
    )
```
